8 devices in a mesh: dp: 1 (over z), tp: 2 (over y), ep: 4 (over x, core).
Axes of the slice: x: 2, y: 2, z: 1, core: 2. Of those that a mesh axis runs over, the one named last changes fastest.
Arguments:
- x_in: bfloat16 [2048, 1536], P(('dp', 'ep', 'tp'))
- norm_gain: bfloat16 [1536], replicated
- w_router: bfloat16 [1536, 40], replicated
- expert_idx: int32 [2048, 8], P(('dp', 'ep', 'tp'))
- w_gate: bfloat16 [40, 1536, 512], P('ep', None, 'tp')
- w_up: bfloat16 [40, 1536, 512], P('ep', None, 'tp')
- w_down: bfloat16 [40, 512, 1536], P('ep', 'tp')
- out_bias: bfloat16 [1536], replicated
- dy_out: bfloat16 [2048, 1536], P(('dp', 'ep', 'tp'))
Outputs:
- output 1: bfloat16 [2048, 1536], P(('dp', 'ep', 'tp'))
- output 2: bfloat16 [2048, 1536], P(('dp', 'ep', 'tp'))
- output 3: float32 [1536], P('dp')
- output 4: float32 [1536, 40], P('dp')
- output 5: float32 [40, 1536, 512], P(('dp', 'ep'), None, 'tp')
- output 6: float32 [40, 1536, 512], P(('dp', 'ep'), None, 'tp')
- output 7: float32 [40, 512, 1536], P(('dp', 'ep'), 'tp')
- output 8: float32 [1536], P('dp')
All inputs are finite; a program needn't handle non-finite values.
Results may differ from the reference program's by a relative error of at most 0.0103545.
Values are sent between devices in bfloat16 or wider.
A program may use at most 1 GiB of HBM per device.

```python
import jax
import jax.numpy as jnp
from jax import lax

TOK = 256
D = 1536
FF = 512
EXPERTS = 40
TOP = 8
EP_DEVS = 4
TP_DEVS = 2
CAP = 103
EPS = 1e-6


def permute_tokens(perm_key):
    return jax.random.permutation(perm_key, TOK)


def draw_routing(route_key):
    n_src = EP_DEVS * TP_DEVS
    key_heavy, key_weight, key_perm = jax.random.split(route_key, 3)
    expert_row = jnp.arange(EXPERTS)[None, :]
    heavy = jax.random.randint(key_heavy, (n_src, 1), 0, EXPERTS)
    is_heavy = expert_row == heavy
    weights = jnp.where(is_heavy, 0, jax.random.randint(key_weight, (n_src, EXPERTS), 2, 5))
    rest = TOK * TOP - CAP
    share = rest * weights // jnp.sum(weights, axis=1, keepdims=True)
    left_over = rest - jnp.sum(share, axis=1, keepdims=True)
    light_rank = jnp.cumsum(jnp.where(is_heavy, 0, 1), axis=1) - 1
    extra = jnp.where(jnp.logical_and(jnp.logical_not(is_heavy), light_rank < left_over), 1, 0)
    counts = jnp.where(is_heavy, CAP, share + extra)
    ends = jnp.cumsum(counts, axis=1)
    position = jnp.arange(TOP)[None, :] * TOK + jnp.arange(TOK)[:, None]
    choice = jnp.sum((position[None, :, :, None] >= ends[:, None, None, :]).astype(jnp.int32), axis=-1)
    perms = jax.vmap(permute_tokens)(jax.random.split(key_perm, n_src))
    choice = jnp.take_along_axis(choice, perms[:, :, None], axis=1)
    return choice.reshape(n_src * TOK, TOP).astype(jnp.int32)


def setup_inputs(seed: int = 0, part: int = 0) -> dict:
    part_key = jax.random.fold_in(jax.random.key(seed), part)
    key_x, key_dy, key_route = jax.random.split(part_key, 3)
    key_g, key_r, key_wg, key_wu, key_wd, key_b = jax.random.split(jax.random.key(seed + 1), 6)
    n_rows = EP_DEVS * TP_DEVS * TOK
    x_in = jax.random.normal(key_x, (n_rows, D), jnp.float32).astype(jnp.bfloat16)
    norm_gain = (1.0 + 0.3 * jax.random.normal(key_g, (D,), jnp.float32)).astype(jnp.bfloat16)
    w_router = (2.0 * D ** -0.5 * jax.random.normal(key_r, (D, EXPERTS), jnp.float32)).astype(jnp.bfloat16)
    w_gate = (D ** -0.5 * jax.random.normal(key_wg, (EXPERTS, D, FF), jnp.float32)).astype(jnp.bfloat16)
    w_up = (D ** -0.5 * jax.random.normal(key_wu, (EXPERTS, D, FF), jnp.float32)).astype(jnp.bfloat16)
    w_down = (1.5 * FF ** -0.5 * jax.random.normal(key_wd, (EXPERTS, FF, D), jnp.float32)).astype(jnp.bfloat16)
    out_bias = (0.5 * jax.random.normal(key_b, (D,), jnp.float32)).astype(jnp.bfloat16)
    dy_out = jax.random.normal(key_dy, (n_rows, D), jnp.float32).astype(jnp.bfloat16)
    expert_idx = draw_routing(key_route)
    return {"x_in": x_in, "norm_gain": norm_gain, "w_router": w_router, "expert_idx": expert_idx, "w_gate": w_gate, "w_up": w_up, "w_down": w_down, "out_bias": out_bias, "dy_out": dy_out}


def to_bf16(values):
    return values + lax.stop_gradient(values.astype(jnp.bfloat16).astype(jnp.float32) - values)


def reference(x_in, norm_gain, w_router, expert_idx, w_gate, w_up, w_down, out_bias, dy_out):
    n_rows = x_in.shape[0]
    rows_max = EP_DEVS * TP_DEVS * CAP
    flat_ids = expert_idx.reshape(-1)
    order = jnp.argsort(flat_ids, stable=True)
    counts = jnp.sum((flat_ids[:, None] == jnp.arange(EXPERTS)[None, :]).astype(jnp.int32), axis=0)
    starts = jnp.cumsum(counts) - counts
    slot_rank = jnp.arange(rows_max)[None, :]
    slot_tok = order[jnp.minimum(starts[:, None] + slot_rank, n_rows * TOP - 1)] // TOP
    slot_ok = slot_rank < counts[:, None]
    copy_pos = (flat_ids * rows_max + jnp.argsort(order) - starts[flat_ids]).reshape(n_rows, TOP)

    def forward(x_f32, gain, router, gate_w, up_w, down_w, bias):
        inv_rms = lax.rsqrt(jnp.mean(x_f32 * x_f32, axis=-1, keepdims=True) + EPS)
        hidden = to_bf16(x_f32 * inv_rms * gain)
        logits = jnp.dot(hidden, router, preferred_element_type=jnp.float32)
        gates = jax.nn.softmax(jnp.take_along_axis(logits, expert_idx, axis=1), axis=-1)

        def one_expert(operands):
            gate_e, up_e, down_e, tok_e, ok_e = operands
            rows_in = jnp.where(ok_e[:, None], hidden[tok_e], 0.0)
            gate_pre = jnp.dot(rows_in, gate_e, preferred_element_type=jnp.float32)
            up_pre = jnp.dot(rows_in, up_e, preferred_element_type=jnp.float32)
            hidden_act = to_bf16(jax.nn.silu(gate_pre) * up_pre)
            return to_bf16(jnp.dot(hidden_act, down_e, preferred_element_type=jnp.float32))

        y_slots = lax.map(jax.checkpoint(one_expert), (gate_w, up_w, down_w, slot_tok, slot_ok))
        y_copy = y_slots.reshape(EXPERTS * rows_max, D)[copy_pos]
        return x_f32 + jnp.sum(gates[:, :, None] * y_copy, axis=1) + bias

    y_f32, pullback = jax.vjp(forward, x_in.astype(jnp.float32), norm_gain.astype(jnp.float32), w_router.astype(jnp.float32), w_gate.astype(jnp.float32), w_up.astype(jnp.float32), w_down.astype(jnp.float32), out_bias.astype(jnp.float32))
    cotangents = pullback(dy_out.astype(jnp.float32))
    return (y_f32.astype(jnp.bfloat16), cotangents[0].astype(jnp.bfloat16), cotangents[1], cotangents[2], cotangents[3], cotangents[4], cotangents[5], cotangents[6])
```

```python
import functools

import jax
import jax.numpy as jnp
from jax import lax
from jax.experimental import pallas as pl
from jax.experimental.pallas import tpu as pltpu
from jax.sharding import PartitionSpec as P

EPS = 1e-6
F32 = jnp.float32
BF16 = jnp.bfloat16
LANES = 128
MIB = 1 << 20


def dot(a, b):
    return jnp.dot(a, b, preferred_element_type=F32)


def dot_nt(a, b):
    return lax.dot_general(a, b, (((1,), (1,)), ((), ())), preferred_element_type=F32)


def dot_tn(a, b):
    return lax.dot_general(a, b, (((0,), (0,)), ((), ())), preferred_element_type=F32)


def split3(value):
    high = value.astype(BF16).astype(F32)
    rest = value - high
    middle = rest.astype(BF16).astype(F32)
    return high, middle, rest - middle


def band_pick(lane, n_exp, parts):
    high, middle, low = parts
    return jnp.where(lane < n_exp, high, jnp.where(lane < 2 * n_exp, middle, low))


def norm_stats(x_f32):
    return lax.rsqrt(jnp.mean(x_f32 * x_f32, axis=-1, keepdims=True) + EPS)


def prologue_body(n_exp, x_ref, gain_ref, router_ref, idx_ref, dy_ref, pack_ref):
    rows, d_model = x_ref.shape
    x_f32 = x_ref[...].astype(F32)
    hidden = (x_f32 * norm_stats(x_f32) * gain_ref[...].astype(F32)).astype(BF16)
    pack_ref[:, :d_model] = hidden
    pack_ref[:, d_model : 2 * d_model] = dy_ref[...]
    logits = dot(hidden, router_ref[...])
    lane = lax.broadcasted_iota(jnp.int32, (rows, LANES), 1)
    expert = jnp.where(lane < n_exp, lane, jnp.where(lane < 2 * n_exp, lane - n_exp, lane - 2 * n_exp))
    chosen = jnp.zeros((rows, LANES), F32)
    for j in range(idx_ref.shape[1]):
        chosen = jnp.where(idx_ref[:, j : j + 1] == expert, 1.0, chosen)
    top = jnp.max(jnp.where(chosen > 0, logits, -jnp.inf), axis=-1, keepdims=True)
    weight = jnp.where(chosen > 0, jnp.exp(jnp.where(chosen > 0, logits - top, 0.0)), 0.0)
    total = jnp.sum(jnp.where(lane < n_exp, weight, 0.0), axis=-1, keepdims=True)
    gates = jnp.where(chosen > 0, weight / total, -1.0)
    bands = jnp.where(lane < 3 * n_exp, band_pick(lane, n_exp, split3(gates)), 0.0)
    pack_ref[:, 2 * d_model :] = bands.astype(BF16)


def prologue(x_in, gain, router3, idx, dy, n_exp):
    rows, d_model = x_in.shape
    block = 64
    return pl.pallas_call(
        functools.partial(prologue_body, n_exp),
        grid=(rows // block,),
        in_specs=[
            pl.BlockSpec((block, d_model), lambda i: (i, 0)),
            pl.BlockSpec((1, d_model), lambda i: (0, 0)),
            pl.BlockSpec((d_model, LANES), lambda i: (0, 0)),
            pl.BlockSpec((block, idx.shape[1]), lambda i: (i, 0)),
            pl.BlockSpec((block, d_model), lambda i: (i, 0)),
        ],
        out_specs=pl.BlockSpec((block, 2 * d_model + LANES), lambda i: (i, 0)),
        out_shape=jax.ShapeDtypeStruct((rows, 2 * d_model + LANES), BF16),
        cost_estimate=pl.CostEstimate(flops=200_000_000, bytes_accessed=3 * rows * d_model * 2, transcendentals=0),
        name="prologue",
    )(x_in, gain, router3, idx, dy)


def expert_body(n_exp, n_local, chained, place, *refs):
    if chained:
        place_ref, near, far, w_gate, w_up, w_down, _, _, out_near, out_far, rows_ref, cot_ref = refs[:12]
    else:
        place_ref, near, far, w_gate, w_up, w_down, out_near, out_far, rows_ref, cot_ref = refs[:10]
    held, gate_t, rank_t, back, total, sem = refs[-6:]
    step = pl.program_id(0)
    n_tok = held.shape[0]
    half = n_tok // 2
    d_model = w_gate.shape[1]
    width = w_gate.shape[2]
    slots = rows_ref.shape[1]

    @pl.when(step == 0)
    def _():
        first = pltpu.make_async_copy(near, held.at[pl.ds(0, half)], sem.at[0])
        second = pltpu.make_async_copy(far, held.at[pl.ds(half, half)], sem.at[1])
        first.start()
        second.start()
        total[...] = jnp.zeros_like(total)
        first.wait()
        second.wait()
        bands = held[:, 2 * d_model :].astype(F32).T
        gates = bands[:n_exp] + bands[n_exp : 2 * n_exp] + bands[2 * n_exp : 3 * n_exp]
        chosen = gates >= 0
        before = lax.broadcasted_iota(jnp.int32, (n_tok, n_tok), 0) < lax.broadcasted_iota(jnp.int32, (n_tok, n_tok), 1)
        rank = dot(jnp.where(chosen, 1.0, 0.0).astype(BF16), jnp.where(before, 1.0, 0.0).astype(BF16))
        gate_t[...] = gates
        rank_t[...] = jnp.where(chosen, rank, -1.0)

    expert = place_ref[0] * n_local + step
    rank = rank_t[pl.ds(expert, 1), :]
    gate = gate_t[pl.ds(expert, 1), :]
    slot = lax.broadcasted_iota(jnp.int32, (slots, n_tok), 0).astype(F32)
    here = slot == rank
    pick = jnp.where(here, 1.0, 0.0).astype(BF16)
    gate_row = jnp.sum(jnp.where(here, gate, 0.0), axis=1, keepdims=True)
    for start in range(0, 2 * d_model, 512):
        rows_ref[0, :, start : start + 512] = dot(pick, held[:, start : start + 512]).astype(BF16)
    rows = rows_ref[0, :, :d_model]
    gate_pre = dot(rows, w_gate[0])
    up_pre = dot(rows, w_up[0])
    down_cot = dot_nt(rows_ref[0, :, d_model:], w_down[0])
    sigma = jax.nn.sigmoid(gate_pre)
    silu = gate_pre * sigma
    act = (silu * up_pre).astype(BF16)
    act_f32 = act.astype(F32)
    d_gate_row = jnp.sum(act_f32 * down_cot, axis=1, keepdims=True)
    d_act = gate_row * down_cot
    d_gate_pre = (d_act * up_pre * sigma * (1.0 + gate_pre * (1.0 - sigma))).astype(BF16)
    d_up_pre = (d_act * silu).astype(BF16)
    cot_ref[0, :, :width] = d_gate_pre
    cot_ref[0, :, width : 2 * width] = d_up_pre
    cot_ref[0, :, 2 * width :] = (gate_row * act_f32).astype(BF16)
    for start in range(0, d_model, 512):
        cols = slice(start, start + 512)
        back[:, cols] = (gate_row * dot(act, w_down[0, :, cols])).astype(BF16)
        back[:, d_model + start : d_model + start + 512] = (dot_nt(d_gate_pre, w_gate[0, cols, :]) + dot_nt(d_up_pre, w_up[0, cols, :])).astype(BF16)
    lane = lax.broadcasted_iota(jnp.int32, (slots, LANES), 1)
    mine = jnp.logical_or(jnp.logical_or(lane == expert, lane == expert + n_exp), lane == expert + 2 * n_exp)
    back[:, 2 * d_model :] = jnp.where(mine, band_pick(lane, n_exp, split3(d_gate_row)), 0.0).astype(BF16)
    for start in range(0, 2 * d_model + LANES, 640):
        cols = slice(start, start + 640)
        total[:, cols] += dot_tn(pick, back[:, cols])

    @pl.when(step == n_local - 1)
    def _():
        out_near[...] = total[:half].astype(BF16)
        out_far[...] = total[half:].astype(BF16)


def expert_chunk(place, near, far, w_gate, w_up, w_down, n_exp, slots, n_chunks, chunk, saved):
    half, packed = near.shape
    n_local, d_model, width = w_gate.shape
    chained = saved is not None
    any_spec = pl.BlockSpec(memory_space=pl.ANY)
    in_specs = [
        any_spec,
        any_spec,
        pl.BlockSpec((1, d_model, width), lambda i, p: (i, 0, 0)),
        pl.BlockSpec((1, d_model, width), lambda i, p: (i, 0, 0)),
        pl.BlockSpec((1, width, d_model), lambda i, p: (i, 0, 0)),
    ]
    operands = [place, near, far, w_gate, w_up, w_down]
    aliases = {}
    if chained:
        in_specs += [any_spec, any_spec]
        aliases = {6: 2, 7: 3}
        operands += list(saved)
    flat = jax.ShapeDtypeStruct((half, packed), BF16)
    flops = n_local * slots * 2 * d_model * (6 * width + 4 * 2 * half)
    return pl.pallas_call(
        functools.partial(expert_body, n_exp, n_local, chained, None),
        grid_spec=pltpu.PrefetchScalarGridSpec(
            num_scalar_prefetch=1,
            grid=(n_local,),
            in_specs=in_specs,
            out_specs=[
                pl.BlockSpec((half, packed), lambda i, p: (0, 0)),
                pl.BlockSpec((half, packed), lambda i, p: (0, 0)),
                pl.BlockSpec((1, slots, 2 * d_model), lambda i, p: (i, chunk, 0)),
                pl.BlockSpec((1, slots, 3 * width), lambda i, p: (i, chunk, 0)),
            ],
            scratch_shapes=[
                pltpu.VMEM((2 * half, packed), BF16),
                pltpu.VMEM((n_exp, 2 * half), F32),
                pltpu.VMEM((n_exp, 2 * half), F32),
                pltpu.VMEM((slots, packed), BF16),
                pltpu.VMEM((2 * half, packed), F32),
                pltpu.SemaphoreType.DMA((2,)),
            ],
        ),
        out_shape=[
            flat,
            flat,
            jax.ShapeDtypeStruct((n_local, n_chunks * slots, 2 * d_model), BF16),
            jax.ShapeDtypeStruct((n_local, n_chunks * slots, 3 * width), BF16),
        ],
        input_output_aliases=aliases,
        compiler_params=pltpu.CompilerParams(dimension_semantics=("arbitrary",), vmem_limit_bytes=60 * MIB),
        cost_estimate=pl.CostEstimate(flops=flops, bytes_accessed=40 * MIB, transcendentals=0),
        name=f"experts_{chunk}",
    )(*operands)


def grads_body(rows_ref, cot_ref, d_gate, d_up, d_down):
    d_model = d_gate.shape[1]
    width = d_gate.shape[2]
    for start in range(0, d_model, 512):
        cols = slice(start, start + 512)
        pair = dot_tn(rows_ref[0, :, cols], cot_ref[0, :, : 2 * width])
        d_gate[0, cols, :] = pair[:, :width]
        d_up[0, cols, :] = pair[:, width:]
        d_down[0, :, cols] = dot_tn(cot_ref[0, :, 2 * width :], rows_ref[0, :, d_model + start : d_model + start + 512])


def weight_grads(rows, cots, first, count):
    _, n_rows, wide = rows.shape
    d_model = wide // 2
    width = cots.shape[2] // 3
    flops = count * n_rows * 2 * d_model * 3 * width
    return pl.pallas_call(
        grads_body,
        grid=(count,),
        in_specs=[
            pl.BlockSpec((1, n_rows, wide), lambda i: (first + i, 0, 0)),
            pl.BlockSpec((1, n_rows, 3 * width), lambda i: (first + i, 0, 0)),
        ],
        out_specs=[
            pl.BlockSpec((1, d_model, width), lambda i: (i, 0, 0)),
            pl.BlockSpec((1, d_model, width), lambda i: (i, 0, 0)),
            pl.BlockSpec((1, width, d_model), lambda i: (i, 0, 0)),
        ],
        out_shape=[
            jax.ShapeDtypeStruct((count, d_model, width), F32),
            jax.ShapeDtypeStruct((count, d_model, width), F32),
            jax.ShapeDtypeStruct((count, width, d_model), F32),
        ],
        compiler_params=pltpu.CompilerParams(dimension_semantics=("arbitrary",), vmem_limit_bytes=60 * MIB),
        cost_estimate=pl.CostEstimate(flops=flops, bytes_accessed=90 * MIB, transcendentals=0),
        name="weight_grads",
    )(rows, cots)


def epilogue_body(n_exp, x_ref, gain_ref, router_ref, bias_ref, pack_ref, p0, p1, p2, p3, p4, y_ref, dx_ref, stat_ref):
    rows, d_model = x_ref.shape
    parts = (p0, p1, p2, p3, p4)
    x_f32 = x_ref[...].astype(F32)
    dy_f32 = pack_ref[:, d_model : 2 * d_model].astype(F32)
    hidden = pack_ref[:, :d_model]
    inv_rms = norm_stats(x_f32)
    normed = x_f32 * inv_rms
    moe_out = sum(p[:, :d_model].astype(F32) for p in parts)
    y_ref[...] = (x_f32 + (moe_out + bias_ref[...].astype(F32))).astype(BF16)
    band = lax.broadcasted_iota(jnp.int32, (LANES, LANES), 0)
    col = lax.broadcasted_iota(jnp.int32, (LANES, LANES), 1)
    match = jnp.logical_or(jnp.logical_or(band == col, band == col + n_exp), band == col + 2 * n_exp)
    fold = jnp.where(jnp.logical_and(match, col < n_exp), 1.0, 0.0).astype(BF16)
    gates = jnp.maximum(dot(pack_ref[:, 2 * d_model :], fold), 0.0)
    d_gates = sum(dot(p[:, 2 * d_model :], fold) for p in parts)
    d_logits = (gates * (d_gates - jnp.sum(gates * d_gates, axis=-1, keepdims=True))).astype(BF16)
    d_router_t = dot_tn(d_logits, hidden)
    dh = sum(p[:, d_model : 2 * d_model].astype(F32) for p in parts) + dot_nt(d_logits, router_ref[...])
    d_gain = jnp.sum(dh * normed, axis=0, keepdims=True)
    d_bias = jnp.sum(dy_f32, axis=0, keepdims=True)
    d_norm = dh * gain_ref[...].astype(F32)
    dx_ref[...] = (dy_f32 + inv_rms * (d_norm - normed * jnp.mean(d_norm * normed, axis=-1, keepdims=True))).astype(BF16)
    which = lax.broadcasted_iota(jnp.int32, (8, d_model), 0)
    tail = jnp.where(which == 0, d_gain, jnp.where(which == 1, d_bias, 0.0))

    @pl.when(pl.program_id(0) == 0)
    def _():
        stat_ref[...] = jnp.zeros_like(stat_ref)

    stat_ref[:n_exp, :] += d_router_t[:n_exp]
    stat_ref[n_exp:, :] += tail


def epilogue(x_in, gain, router3, bias, pack, parts, n_exp):
    rows, d_model = x_in.shape
    packed = pack.shape[1]
    block = 64
    row_spec = pl.BlockSpec((block, d_model), lambda i: (i, 0))
    vec_spec = pl.BlockSpec((1, d_model), lambda i: (0, 0))
    pack_spec = pl.BlockSpec((block, packed), lambda i: (i, 0))
    return pl.pallas_call(
        functools.partial(epilogue_body, n_exp),
        grid=(rows // block,),
        in_specs=[row_spec, vec_spec, pl.BlockSpec((d_model, LANES), lambda i: (0, 0)), vec_spec] + [pack_spec] * 6,
        out_specs=[row_spec, row_spec, pl.BlockSpec((n_exp + 8, d_model), lambda i: (0, 0))],
        out_shape=[
            jax.ShapeDtypeStruct((rows, d_model), BF16),
            jax.ShapeDtypeStruct((rows, d_model), BF16),
            jax.ShapeDtypeStruct((n_exp + 8, d_model), F32),
        ],
        compiler_params=pltpu.CompilerParams(dimension_semantics=("arbitrary",)),
        cost_estimate=pl.CostEstimate(flops=400_000_000, bytes_accessed=12 * MIB, transcendentals=0),
        name="epilogue",
    )(x_in, gain, router3, bias, pack, *parts)


def solution(mesh):
    tok_spec = P(("dp", "ep", "tp"), None)
    wide_spec = P("ep", None, "tp")
    down_spec = P("ep", "tp", None)
    grad_wide = P(("dp", "ep"), None, "tp")
    grad_down = P(("dp", "ep"), "tp", None)
    n_ep, n_tp = mesh.shape["ep"], mesh.shape["tp"]

    def swap(value, ep_flip, tp_flip):
        pairs = [(t * n_ep + e, (t ^ tp_flip) * n_ep + (e ^ ep_flip)) for t in range(n_tp) for e in range(n_ep)]
        return lax.ppermute(value, ("tp", "ep"), pairs)

    def device_step(x_in, norm_gain, w_router, expert_idx, w_gate, w_up, w_down, out_bias, dy_out):
        n_tok, d_model = x_in.shape
        n_exp = w_router.shape[1]
        top_k = expert_idx.shape[1]
        n_local = w_gate.shape[0]
        capacity = (2 * n_tok * top_k + n_exp - 1) // n_exp
        slots = (2 * capacity + 15) // 16 * 16
        gain = norm_gain.reshape(1, d_model)
        bias = out_bias.reshape(1, d_model)
        router3 = jnp.concatenate([w_router] * 3 + [jnp.zeros((d_model, LANES - 3 * n_exp), BF16)], axis=1)
        pack = prologue(x_in, gain, router3, expert_idx, dy_out, n_exp)
        place = lax.axis_index("ep").astype(jnp.int32).reshape(1)
        flips = ((2, 0), (0, 1), (2, 1))
        n_chunks = 1 + len(flips)
        blocks = [(pack, swap(pack, 1, 0))]
        arrived = [swap(pack, *flip) for flip in flips]
        blocks += [(block, swap(block, 1, 0)) for block in arrived]
        saved = None
        parts = []
        for chunk, (near, far) in enumerate(blocks):
            out_near, out_far, rows, cots = expert_chunk(place, near, far, w_gate, w_up, w_down, n_exp, slots, n_chunks, chunk, saved)
            saved = (rows, cots)
            other = swap(out_far, 1, 0)
            if chunk == 0:
                parts += [out_near, other]
            else:
                pair = (out_near.astype(F32) + other.astype(F32)).astype(BF16)
                parts.append(swap(pair, *flips[chunk - 1]))
        d_gate, d_up, d_down = weight_grads(saved[0], saved[1], 0, n_local)
        y_out, dx_in, stats = epilogue(x_in, gain, router3, bias, pack, parts, n_exp)
        stats = lax.psum(stats, ("ep", "tp"))
        return y_out, dx_in, stats[n_exp], stats[:n_exp].T, d_gate, d_up, d_down, stats[n_exp + 1]

    return jax.shard_map(device_step, mesh=mesh, in_specs=(tok_spec, P(None), P(None, None), tok_spec, wide_spec, wide_spec, down_spec, P(None), tok_spec), out_specs=(tok_spec, tok_spec, P("dp"), P("dp", None), grad_wide, grad_wide, grad_down, P("dp")), check_vma=False)
```
